32 devices in a mesh: sub: 2 (over y), row: 4 (over x, core), col: 4 (over z).
Axes of the slice: x: 2, y: 2, z: 4, core: 2. Of those that a mesh axis runs over, the one named last changes fastest.
Arguments:
- factor_window: bfloat16 [2, 8192, 1024], P('sub', ('row', 'col'))
- right_sides: bfloat16 [2, 8192, 2048], P('sub', 'row', 'col'), may hold values from -1.1953125 to 1.1953125
- first_block: int32 [2, 8], P('sub'), may hold values from 0 to 4
- tile_map: int32 [2, 8], P('sub'), may hold values from 0 to 15, as said below
- interface_block: float32 [4096, 4096], P(('sub', 'row'), 'col'), may hold values from -6 to 6
Outputs:
- updated_sides: bfloat16 [2, 8192, 2048], P('sub', 'row', 'col')
- schur_global: float32 [4096, 4096], P(('sub', 'row'), 'col')
The draws below stay inside these ranges and needn't reach their ends.
Inputs may be any that keep to these rules, and one draw needn't show every extreme that they name: `tile_map`: the 8 entries of a subdomain are different global tiles.
All inputs are finite; a program needn't handle non-finite values.
Results may differ from the reference program's by a relative error of at most 0.0075.
Values may be sent and summed in bfloat16 or wider, within the bound.
A program may use at most 64 MiB of HBM per device.

```python
import math
import jax
import jax.numpy as jnp
from jax import lax

N_INT = 8192
K_IFACE = 2048
PANEL = 256
BLOCK = 256
STEPS = 4
GTILES = 16
WINDOW = 1024
KBLOCKS = 8
GORDER = 4096
N_SUB = 2


def draw_factor_window(key, part):
    key_off, key_diag = jax.random.split(jax.random.fold_in(key, 11))
    scale = 0.6 / math.sqrt(WINDOW)
    off_diag = jax.random.normal(key_off, (N_SUB, N_INT, WINDOW), jnp.float32) * scale
    diagonal = jnp.exp(jax.random.uniform(key_diag, (N_SUB, N_INT, 1), jnp.float32, 0.0, math.log(2.0)))
    row_index = jnp.arange(N_INT, dtype=jnp.int32)[:, None]
    col_index = jnp.arange(WINDOW, dtype=jnp.int32)[None, :]
    lower = jnp.where(row_index > col_index, off_diag, jnp.float32(0.0))
    factor = jnp.where(row_index == col_index, diagonal, lower)
    return factor.astype(jnp.bfloat16)


def draw_tile_map(key, part):
    keys = jax.random.split(jax.random.fold_in(key, 23), N_SUB)

    def pick(single):
        return jax.random.permutation(single, GTILES)[:KBLOCKS]
    return jax.vmap(pick)(keys).astype(jnp.int32)


def with_ends(result, stream_key, least, top_value):
    longest = result.shape.index(max(result.shape))
    spots = []
    for shift in (0, 1):
        where = [jax.random.randint(jax.random.fold_in(stream_key, axis), (), 0, length) for axis, length in enumerate(result.shape)]
        where[longest] = (where[longest] + shift) % result.shape[longest]
        spots.append(tuple(where))
    return result.at[spots[0]].set(least).at[spots[1]].set(top_value)


def level_of(stream_key, dims, shards, smallest, top_value):
    factor_of = 1.0
    for position, blocks in shards:
        heights = jax.random.uniform(jax.random.fold_in(jax.random.fold_in(stream_key, 6), position), (blocks,), jnp.float32, smallest / len(shards), top_value / len(shards))
        factor_of = factor_of * jnp.repeat(jnp.exp(heights), dims[position] // blocks).reshape((-1,) + (1,) * (len(dims) - 1 - position))
    return factor_of


def scatter_about(key, dims, width, limit, shards=(), held_as=jnp.bfloat16):
    array = jax.random.normal(key, dims, jnp.float32) * width
    if len(shards) > 0:
        array = level_of(key, dims, shards, -0.22, 0.18) * array
    return jnp.clip(array, min=-limit, max=limit).astype(held_as)


def setup_inputs(seed: int = 0) -> dict:
    seeds = jax.random.split(jax.random.key(seed), 6)
    return {
        "factor_window": draw_factor_window(jax.random.fold_in(seeds[5], 71), 0),
        "right_sides": scatter_about(seeds[1], (N_SUB, N_INT, K_IFACE), 0.2, 1.1953125, ((0, 2), (1, 4), (2, 4))),
        "first_block": with_ends(jax.random.randint(seeds[2], (N_SUB, KBLOCKS), 0, STEPS + 1), jax.random.fold_in(seeds[2], 1), 0, STEPS).astype(jnp.int32),
        "tile_map": draw_tile_map(jax.random.fold_in(seeds[5], 71), 0),
        "interface_block": scatter_about(seeds[4], (GORDER, GORDER), 1.0, 6.0, ((0, 8), (1, 4)), jnp.float32),
    }


def reference(factor_window, right_sides, first_block, tile_map, interface_block):
    total = jnp.zeros((GORDER, GORDER), jnp.float32)
    row_index = jnp.arange(N_INT, dtype=jnp.int32)
    col_block = jnp.arange(K_IFACE, dtype=jnp.int32) // BLOCK
    outputs = []
    for subdomain in range(N_SUB):
        factor = factor_window[subdomain]
        first_col = first_block[subdomain][col_block]
        live = (row_index // PANEL)[:, None] >= first_col[None, :]
        current = jnp.where(live, right_sides[subdomain].astype(jnp.float32), jnp.float32(0.0))
        pieces = []
        for panel in range(STEPS):
            offset = panel * PANEL
            diag_block = factor[offset:offset + PANEL, offset:offset + PANEL].astype(jnp.float32)
            solved = jax.scipy.linalg.solve_triangular(diag_block, current[offset:offset + PANEL], lower=True).astype(jnp.bfloat16)
            update = jnp.dot(factor[:, offset:offset + PANEL].astype(jnp.float32), solved.astype(jnp.float32), preferred_element_type=jnp.float32)
            current = jnp.where((row_index >= offset + PANEL)[:, None], current - update, current)
            current = current.at[offset:offset + PANEL].set(solved.astype(jnp.float32))
            pieces.append(solved)
        outputs.append(current.astype(jnp.bfloat16))
        stacked = jnp.concatenate(pieces, axis=0).astype(jnp.float32)
        onehot = (tile_map[subdomain][:, None] == jnp.arange(GTILES, dtype=jnp.int32)[None, :]).astype(jnp.float32)
        spread = jnp.einsum('wbj,bg->wgj', stacked.reshape(WINDOW, KBLOCKS, BLOCK), onehot, precision=lax.Precision.HIGHEST).reshape(WINDOW, GORDER)
        total = total + jnp.dot(spread.T, spread, precision=lax.Precision.HIGHEST)
    schur_global = interface_block - total
    return (jnp.stack(outputs, axis=0), schur_global)
```

```python
import functools
import math

import jax
import jax.numpy as jnp
from jax import lax
from jax.experimental import pallas as pl
from jax.experimental.pallas import tpu as pltpu
from jax.sharding import PartitionSpec as P

PANEL = 256
BLOCK = 256
STEPS = 4
GTILES = 16
TINY = 16
EXACT = lax.Precision.HIGHEST


def iota(shape, dim):
    return lax.broadcasted_iota(jnp.int32, shape, dim)


def invert(diag):
    n = diag.shape[0]
    rows, cols = iota((n, n), 0), iota((n, n), 1)
    lower = jnp.where(rows >= cols, diag.astype(jnp.float32), 0.0)
    same = (rows >> 4) == (cols >> 4)
    fold = jnp.where((iota((n, 128), 0) & (TINY - 1)) == iota((n, 128), 1), 1.0, 0.0)
    compact = jnp.dot(
        jnp.where(same, lower, 0.0).astype(jnp.bfloat16),
        fold.astype(jnp.bfloat16),
        preferred_element_type=jnp.float32,
    )
    a = compact.reshape(n // TINY, TINY, 128)
    y = fold.reshape(n // TINY, TINY, 128)
    place = iota(y.shape, 1)
    for j in range(TINY):
        pivot = y[:, j : j + 1, :] / a[:, j : j + 1, j : j + 1]
        y = jnp.where(place == j, pivot, jnp.where(place > j, y - a[:, :, j : j + 1] * pivot, y))
    full = lax.dot_general(
        y.reshape(n, 128),
        fold,
        (((1,), (1,)), ((), ())),
        precision=EXACT,
        preferred_element_type=jnp.float32,
    )
    inverse = jnp.where(same, full, 0.0)
    level = 4
    while (1 << level) < n:
        off = ((rows >> (level + 1)) == (cols >> (level + 1))) & ((rows >> level) != (cols >> level))
        inner = jnp.dot(
            jnp.where(off, lower, 0.0), inverse, precision=EXACT, preferred_element_type=jnp.float32
        )
        inverse = inverse - jnp.dot(
            inverse, inner, precision=EXACT, preferred_element_type=jnp.float32
        )
        level += 1
    return inverse


def solve_kernel(first_ref, l_ref, r_ref, x_ref):
    for p in range(STEPS):
        at = slice(p * PANEL, (p + 1) * PANEL)
        inverse = invert(l_ref[at, at])
        right = jnp.where(first_ref[...] <= p, r_ref[at, :].astype(jnp.float32), 0.0)
        if p:
            right = right - jnp.dot(
                l_ref[at, : p * PANEL], x_ref[: p * PANEL, :], preferred_element_type=jnp.float32
            )
        x_ref[at, :] = jnp.dot(
            inverse, right, precision=EXACT, preferred_element_type=jnp.float32
        ).astype(jnp.bfloat16)


def solve(first_col, factor_rows, sides):
    window, bc = factor_rows.shape[1], sides.shape[1]
    return pl.pallas_call(
        solve_kernel,
        out_shape=jax.ShapeDtypeStruct((window, bc), jnp.bfloat16),
        grid=(1,),
        in_specs=[
            pl.BlockSpec((1, bc), lambda i: (0, 0)),
            pl.BlockSpec((window, window), lambda i: (0, 0)),
            pl.BlockSpec((window, bc), lambda i: (0, 0)),
        ],
        out_specs=pl.BlockSpec((window, bc), lambda i: (0, 0)),
        compiler_params=pltpu.CompilerParams(vmem_limit_bytes=48 * 1024 * 1024),
        cost_estimate=pl.CostEstimate(flops=10**10, bytes_accessed=4 * 2**20, transcendentals=0),
    )(first_col, factor_rows, sides)


def schur_kernel(ni, ch, row_src, col_src, *refs):
    a_refs, (b_ref, i_ref, o_ref) = refs[:ni], refs[ni:]
    s, j = pl.program_id(0), pl.program_id(1)

    @pl.when((s == 0) & (j == 0))
    def _():
        o_ref[...] = i_ref[...]

    at = pl.ds(pl.multiple_of(j * ch, ch), ch)
    for i in range(ni):

        @pl.when((row_src[s, i] >= 0) & (col_src[s, j] >= 0))
        def _(i=i):
            a = a_refs[i][0, :, 0].reshape(-1, ch)
            b = b_ref[0, :, 0].reshape(-1, ch)
            term = lax.dot_general(
                a, b, (((0,), (0,)), ((), ())), preferred_element_type=jnp.float32
            )
            o_ref[i * ch : (i + 1) * ch, at] -= term


def schur(full, interface, row_src, col_src, ch):
    subs, rows, _, share, bc = full.shape
    out_rows, out_cols = interface.shape
    ni, nj, per = out_rows // ch, out_cols // ch, bc // ch
    block = (1, rows, 1, share, ch)

    def place(src):
        src = jnp.maximum(src, 0)
        return src // per, src % per

    def a_map(i, s, j, rs, cs):
        c, k = place(rs[s, i])
        return (s, 0, c, 0, k)

    def b_map(s, j, rs, cs):
        c, k = place(cs[s, j])
        return (s, 0, c, 0, k)

    whole = pl.BlockSpec((out_rows, out_cols), lambda s, j, rs, cs: (0, 0))
    return pl.pallas_call(
        functools.partial(schur_kernel, ni, ch),
        out_shape=jax.ShapeDtypeStruct((out_rows, out_cols), jnp.float32),
        grid_spec=pltpu.PrefetchScalarGridSpec(
            num_scalar_prefetch=2,
            grid=(subs, nj),
            in_specs=[pl.BlockSpec(block, functools.partial(a_map, i)) for i in range(ni)]
            + [pl.BlockSpec(block, b_map), whole],
            out_specs=whole,
        ),
        compiler_params=pltpu.CompilerParams(vmem_limit_bytes=48 * 1024 * 1024),
        cost_estimate=pl.CostEstimate(flops=4 * 10**9, bytes_accessed=10 * 2**20, transcendentals=0),
    )(row_src, col_src, *([full] * (ni + 1)), interface)


def chunk_sources(tile_maps, ch):
    count = tile_maps.shape[1]
    hit = tile_maps[:, None, :] == jnp.arange(GTILES, dtype=jnp.int32)[None, :, None]
    block = jnp.sum(jnp.where(hit, jnp.arange(count, dtype=jnp.int32) + 1, 0), axis=2) - 1
    parts = BLOCK // ch
    pieces = block[:, :, None] * parts + jnp.arange(parts, dtype=jnp.int32)
    return jnp.where(block[:, :, None] >= 0, pieces, -1).reshape(tile_maps.shape[0], -1)


def local(factor_window, right_sides, first_block, tile_map, interface_block):
    subs, rows, cols = lax.axis_size("sub"), lax.axis_size("row"), lax.axis_size("col")
    sub_pos, row_pos, col_pos = (lax.axis_index(a) for a in ("sub", "row", "col"))
    sides = right_sides[0]
    block_rows, bc = sides.shape
    window = factor_window.shape[2]
    out_rows, out_cols = interface_block.shape
    is_root = row_pos == 0
    tile_maps = lax.all_gather(tile_map, "sub", axis=0, tiled=True)
    ch = math.gcd(math.gcd(BLOCK, bc), math.gcd(out_rows, out_cols))
    src = chunk_sources(tile_maps, ch)
    row_src = lax.dynamic_slice_in_dim(
        src, (sub_pos * rows + row_pos) * (out_rows // ch), out_rows // ch, 1
    )
    col_src = lax.dynamic_slice_in_dim(src, col_pos * (out_cols // ch), out_cols // ch, 1)

    col_block = (col_pos * bc + jnp.arange(bc, dtype=jnp.int32)) // BLOCK
    ids = jnp.arange(first_block.shape[1], dtype=jnp.int32)
    first_col = jnp.sum(
        jnp.where(col_block[:, None] == ids[None, :], first_block[0][None, :], 0), axis=1
    )[None, :]

    factor_rows = lax.all_gather(factor_window[0], "col", axis=0, tiled=True)
    solved = solve(first_col, factor_rows, sides)
    share = window // rows
    mine = solved[:share]
    for r in range(1, rows):
        sent = lax.ppermute(solved[r * share : (r + 1) * share], "row", [(0, r)])
        mine = jnp.where(row_pos == r, sent, mine)
    full = lax.all_gather(mine, ("sub", "row", "col"), axis=0).reshape(
        subs, rows, cols, share, bc
    )
    own = lax.dynamic_slice(
        full, (sub_pos, 0, col_pos, 0, 0), (1, rows, 1, share, bc)
    ).reshape(window, bc)
    update = jnp.dot(factor_rows, own, preferred_element_type=jnp.float32)
    below = (sides.astype(jnp.float32) - update).astype(jnp.bfloat16)
    in_window = is_root & (jnp.arange(block_rows, dtype=jnp.int32) < window)
    padded = jnp.pad(own, ((0, block_rows - window), (0, 0)))
    updated = jnp.where(in_window[:, None], padded, below)[None]
    return (updated, schur(full, interface_block, row_src, col_src, ch))


def solution(mesh):
    return jax.shard_map(
        local,
        mesh=mesh,
        in_specs=(
            P("sub", ("row", "col"), None),
            P("sub", "row", "col"),
            P("sub", None),
            P("sub", None),
            P(("sub", "row"), "col"),
        ),
        out_specs=(P("sub", "row", "col"), P(("sub", "row"), "col")),
        check_vma=False,
    )
```

```python
import functools
import math

import jax
import jax.numpy as jnp
from jax import lax
from jax.experimental import pallas as pl
from jax.experimental.pallas import tpu as pltpu
from jax.sharding import PartitionSpec as P

PANEL = 256
BLOCK = 256
STEPS = 4
GTILES = 16
TINY = 16
EXACT = lax.Precision.HIGHEST


def iota(shape, dim):
    return lax.broadcasted_iota(jnp.int32, shape, dim)


def invert(diag):
    n = diag.shape[0]
    rows, cols = iota((n, n), 0), iota((n, n), 1)
    lower = jnp.where(rows >= cols, diag.astype(jnp.float32), 0.0)
    same = (rows >> 4) == (cols >> 4)
    fold = jnp.where((iota((n, 128), 0) & (TINY - 1)) == iota((n, 128), 1), 1.0, 0.0)
    compact = jnp.dot(
        jnp.where(same, lower, 0.0).astype(jnp.bfloat16),
        fold.astype(jnp.bfloat16),
        preferred_element_type=jnp.float32,
    )
    a = compact.reshape(n // TINY, TINY, 128)
    y = fold.reshape(n // TINY, TINY, 128)
    place = iota(y.shape, 1)
    for j in range(TINY):
        pivot = y[:, j : j + 1, :] / a[:, j : j + 1, j : j + 1]
        y = jnp.where(place == j, pivot, jnp.where(place > j, y - a[:, :, j : j + 1] * pivot, y))
    full = lax.dot_general(
        y.reshape(n, 128),
        fold,
        (((1,), (1,)), ((), ())),
        precision=EXACT,
        preferred_element_type=jnp.float32,
    )
    inverse = jnp.where(same, full, 0.0)
    level = 4
    while (1 << level) < n:
        off = ((rows >> (level + 1)) == (cols >> (level + 1))) & ((rows >> level) != (cols >> level))
        inner = jnp.dot(
            jnp.where(off, lower, 0.0), inverse, precision=EXACT, preferred_element_type=jnp.float32
        )
        inverse = inverse - jnp.dot(
            inverse, inner, precision=EXACT, preferred_element_type=jnp.float32
        )
        level += 1
    return inverse


def solve_kernel(first_ref, l_ref, r_ref, x_ref):
    for p in range(STEPS):
        at = slice(p * PANEL, (p + 1) * PANEL)
        inverse = invert(l_ref[at, at])
        right = jnp.where(first_ref[...] <= p, r_ref[at, :].astype(jnp.float32), 0.0)
        if p:
            right = right - jnp.dot(
                l_ref[at, : p * PANEL], x_ref[: p * PANEL, :], preferred_element_type=jnp.float32
            )
        x_ref[at, :] = jnp.dot(
            inverse, right, precision=EXACT, preferred_element_type=jnp.float32
        ).astype(jnp.bfloat16)


def solve(first_col, factor_rows, sides):
    window, bc = factor_rows.shape[1], sides.shape[1]
    return pl.pallas_call(
        solve_kernel,
        out_shape=jax.ShapeDtypeStruct((window, bc), jnp.bfloat16),
        grid=(1,),
        in_specs=[
            pl.BlockSpec((1, bc), lambda i: (0, 0)),
            pl.BlockSpec((window, window), lambda i: (0, 0)),
            pl.BlockSpec((window, bc), lambda i: (0, 0)),
        ],
        out_specs=pl.BlockSpec((window, bc), lambda i: (0, 0)),
        compiler_params=pltpu.CompilerParams(vmem_limit_bytes=48 * 1024 * 1024),
        cost_estimate=pl.CostEstimate(flops=10**10, bytes_accessed=4 * 2**20, transcendentals=0),
    )(first_col, factor_rows, sides)


def schur_kernel(ni, ch, row_src, col_src, *refs):
    a_refs, (b_ref, i_ref, o_ref) = refs[:ni], refs[ni:]
    s, j = pl.program_id(0), pl.program_id(1)

    @pl.when((s == 0) & (j == 0))
    def _():
        o_ref[...] = i_ref[...]

    at = pl.ds(pl.multiple_of(j * ch, ch), ch)
    for i in range(ni):

        @pl.when((row_src[s, i] >= 0) & (col_src[s, j] >= 0))
        def _(i=i):
            a = a_refs[i][0, :, 0].reshape(-1, ch)
            b = b_ref[0, :, 0].reshape(-1, ch)
            term = lax.dot_general(
                a, b, (((0,), (0,)), ((), ())), preferred_element_type=jnp.float32
            )
            o_ref[i * ch : (i + 1) * ch, at] -= term


def schur(full, interface, row_src, col_src, ch):
    subs, rows, _, share, bc = full.shape
    out_rows, out_cols = interface.shape
    ni, nj, per = out_rows // ch, out_cols // ch, bc // ch
    block = (1, rows, 1, share, ch)

    def place(src):
        src = jnp.maximum(src, 0)
        return src // per, src % per

    def a_map(i, s, j, rs, cs):
        c, k = place(rs[s, i])
        return (s, 0, c, 0, k)

    def b_map(s, j, rs, cs):
        c, k = place(cs[s, j])
        return (s, 0, c, 0, k)

    whole = pl.BlockSpec((out_rows, out_cols), lambda s, j, rs, cs: (0, 0))
    return pl.pallas_call(
        functools.partial(schur_kernel, ni, ch),
        out_shape=jax.ShapeDtypeStruct((out_rows, out_cols), jnp.float32),
        grid_spec=pltpu.PrefetchScalarGridSpec(
            num_scalar_prefetch=2,
            grid=(subs, nj),
            in_specs=[pl.BlockSpec(block, functools.partial(a_map, i)) for i in range(ni)]
            + [pl.BlockSpec(block, b_map), whole],
            out_specs=whole,
        ),
        compiler_params=pltpu.CompilerParams(vmem_limit_bytes=48 * 1024 * 1024),
        cost_estimate=pl.CostEstimate(flops=4 * 10**9, bytes_accessed=10 * 2**20, transcendentals=0),
    )(row_src, col_src, *([full] * (ni + 1)), interface)


def chunk_sources(tile_maps, ch):
    count = tile_maps.shape[1]
    hit = tile_maps[:, None, :] == jnp.arange(GTILES, dtype=jnp.int32)[None, :, None]
    block = jnp.sum(jnp.where(hit, jnp.arange(count, dtype=jnp.int32) + 1, 0), axis=2) - 1
    parts = BLOCK // ch
    pieces = block[:, :, None] * parts + jnp.arange(parts, dtype=jnp.int32)
    return jnp.where(block[:, :, None] >= 0, pieces, -1).reshape(tile_maps.shape[0], -1)


def local(factor_window, right_sides, first_block, tile_map, interface_block):
    subs, rows, cols = lax.axis_size("sub"), lax.axis_size("row"), lax.axis_size("col")
    sub_pos, row_pos, col_pos = (lax.axis_index(a) for a in ("sub", "row", "col"))
    sides = right_sides[0]
    block_rows, bc = sides.shape
    window = factor_window.shape[2]
    out_rows, out_cols = interface_block.shape
    is_root = row_pos == 0
    tile_maps = lax.all_gather(tile_map, "sub", axis=0, tiled=True)
    ch = math.gcd(math.gcd(BLOCK, bc), math.gcd(out_rows, out_cols))
    src = chunk_sources(tile_maps, ch)
    row_src = lax.dynamic_slice_in_dim(
        src, (sub_pos * rows + row_pos) * (out_rows // ch), out_rows // ch, 1
    )
    col_src = lax.dynamic_slice_in_dim(src, col_pos * (out_cols // ch), out_cols // ch, 1)

    col_block = (col_pos * bc + jnp.arange(bc, dtype=jnp.int32)) // BLOCK
    ids = jnp.arange(first_block.shape[1], dtype=jnp.int32)
    first_col = jnp.sum(
        jnp.where(col_block[:, None] == ids[None, :], first_block[0][None, :], 0), axis=1
    )[None, :]

    factor = factor_window[0]
    height = factor.shape[0]
    holders = window // height
    early = [factor] + [
        lax.ppermute(factor, ("row", "col"), [(h, (h + k) % cols) for h in range(holders)])
        for k in range(1, cols)
    ]
    pieces = []
    for h in range(holders):
        piece = factor
        for k in range(1, cols):
            piece = jnp.where((col_pos - h + cols) % cols == k, early[k], piece)
        pieces.append(piece)
    window_rows = jnp.concatenate(pieces, axis=0)
    factor, window_rows = lax.optimization_barrier((factor, window_rows))
    solved = solve(first_col, window_rows, sides)
    factor_rows = jnp.zeros((cols * height, window), factor.dtype)
    for k in range(cols):
        ring = [(c, (c + k) % cols) for c in range(cols)]
        piece = lax.ppermute(factor, "col", ring) if k else factor
        start = ((col_pos - k + cols) % cols) * height
        factor_rows = lax.dynamic_update_slice(factor_rows, piece, (start, 0))
    share = window // rows
    mine = solved[:share]
    for r in range(1, rows):
        sent = lax.ppermute(solved[r * share : (r + 1) * share], "row", [(0, r)])
        mine = jnp.where(row_pos == r, sent, mine)
    full = lax.all_gather(mine, ("sub", "row", "col"), axis=0).reshape(
        subs, rows, cols, share, bc
    )
    own = lax.dynamic_slice(
        full, (sub_pos, 0, col_pos, 0, 0), (1, rows, 1, share, bc)
    ).reshape(window, bc)
    update = jnp.dot(factor_rows, own, preferred_element_type=jnp.float32)
    below = (sides.astype(jnp.float32) - update).astype(jnp.bfloat16)
    in_window = is_root & (jnp.arange(block_rows, dtype=jnp.int32) < window)
    padded = jnp.pad(own, ((0, block_rows - window), (0, 0)))
    updated = jnp.where(in_window[:, None], padded, below)[None]
    return (updated, schur(full, interface_block, row_src, col_src, ch))


def solution(mesh):
    return jax.shard_map(
        local,
        mesh=mesh,
        in_specs=(
            P("sub", ("row", "col"), None),
            P("sub", "row", "col"),
            P("sub", None),
            P("sub", None),
            P(("sub", "row"), "col"),
        ),
        out_specs=(P("sub", "row", "col"), P(("sub", "row"), "col")),
        check_vma=False,
    )
```
